64 devices in a mesh: videos: 4 (over x, y), frames: 16 (over z, core).
Axes of the slice: x: 2, y: 2, z: 8, core: 2. Of those that a mesh axis runs over, the one named last changes fastest.
The devices are a block of a 4x4x8 slice.
Arguments:
- latents_a: float32 [1024, 256, 4], P(('videos', 'frames')), parts along dimension 0
- mod_a: float32 [1024, 1, 6, 384], P(('videos', 'frames')), parts along dimension 0
- dt_a: float32 [1024], P(('videos', 'frames')), parts along dimension 0
- noise_a: float32 [12, 256, 4], P('videos'), parts along dimension 0
- latents_b: float32 [1024, 256, 4], P(('videos', 'frames')), parts along dimension 0
- mod_b: float32 [1024, 1, 6, 384], P(('videos', 'frames')), parts along dimension 0
- dt_b: float32 [1024], P(('videos', 'frames')), parts along dimension 0
- noise_b: float32 [12, 256, 4], P('videos'), parts along dimension 0
- w_in: bfloat16 [4, 384], replicated
- sp_qkv: bfloat16 [1, 384, 3, 6, 64], replicated
- sp_out: bfloat16 [1, 6, 64, 384], replicated
- tm_qkv: bfloat16 [1, 384, 3, 6, 64], replicated
- tm_bias: float32 [1, 6, 16], replicated
- tm_out: bfloat16 [1, 6, 64, 384], replicated
- mlp_up: bfloat16 [1, 384, 1536], replicated
- mlp_down: bfloat16 [1, 1536, 384], replicated
- w_out: bfloat16 [384, 4], replicated
Outputs:
- output 1: float32 [12, 256, 4], P('videos', 'frames'), parts along dimension 0
- output 2: float32 [1024, 256, 4], P(('videos', 'frames')), parts along dimension 0
- output 3: float32 [12, 256, 4], P('videos', 'frames'), parts along dimension 0
- output 4: float32 [1024, 256, 4], P(('videos', 'frames')), parts along dimension 0
There are 4 independent parts. The reference program is written for one: setup_inputs(seed, part) draws one part's arguments, and reference() takes and returns one part's arrays. A program takes and returns all parts, laid end to end along the dimension named above; an argument that names none is the same for every part.
All inputs are finite; a program needn't handle non-finite values.
Results may differ from the reference program's by a relative error of at most 0.0112564.
Values are sent between devices in bfloat16 or wider.
A program may use at most 768 MiB of HBM per device.

```python
import jax
import jax.numpy as jnp
from jax import lax

MODEL_DIM = 384
NUM_HEADS = 6
FRAME_TOKENS = 256
LATENT_CH = 4
WINDOW = 16
LAYERS = 1
NUM_STEPS = 3
QUEUE_LEN = 256
HEAD_DIM = MODEL_DIM // NUM_HEADS
LN_EPS = 1e-6
MASKED = -1e30


def setup_inputs(seed: int = 0, part: int = 0) -> dict:
    root = jax.random.key(seed)
    shared = jax.random.split(root, 9)
    own = jax.random.split(jax.random.fold_in(root, part), 8)
    qkv_shape = (LAYERS, MODEL_DIM, 3, NUM_HEADS, HEAD_DIM)
    proj_shape = (LAYERS, NUM_HEADS, HEAD_DIM, MODEL_DIM)

    def gaussian(key, shape, scale):
        return jax.random.normal(key, shape, jnp.float32) * scale

    inputs = {}
    for video, first in (('a', 0), ('b', 4)):
        inputs['latents_' + video] = gaussian(own[first], (QUEUE_LEN, FRAME_TOKENS, LATENT_CH), 1.0)
        inputs['mod_' + video] = gaussian(own[first + 1], (QUEUE_LEN, LAYERS, 6, MODEL_DIM), 0.5)
        inputs['dt_' + video] = jax.random.uniform(own[first + 2], (QUEUE_LEN,), jnp.float32, 0.25, 0.5)
        inputs['noise_' + video] = gaussian(own[first + 3], (NUM_STEPS, FRAME_TOKENS, LATENT_CH), 1.0)
    inputs['w_in'] = gaussian(shared[0], (LATENT_CH, MODEL_DIM), LATENT_CH ** -0.5).astype(jnp.bfloat16)
    inputs['sp_qkv'] = gaussian(shared[1], qkv_shape, MODEL_DIM ** -0.5).astype(jnp.bfloat16)
    inputs['sp_out'] = gaussian(shared[2], proj_shape, 2.0 * MODEL_DIM ** -0.5).astype(jnp.bfloat16)
    inputs['tm_qkv'] = gaussian(shared[3], qkv_shape, MODEL_DIM ** -0.5).astype(jnp.bfloat16)
    inputs['tm_bias'] = gaussian(shared[4], (LAYERS, NUM_HEADS, WINDOW), 1.0)
    inputs['tm_out'] = gaussian(shared[5], proj_shape, 2.0 * MODEL_DIM ** -0.5).astype(jnp.bfloat16)
    inputs['mlp_up'] = gaussian(shared[6], (LAYERS, MODEL_DIM, 4 * MODEL_DIM), MODEL_DIM ** -0.5).astype(jnp.bfloat16)
    inputs['mlp_down'] = gaussian(shared[7], (LAYERS, 4 * MODEL_DIM, MODEL_DIM), (4 * MODEL_DIM) ** -0.5).astype(jnp.bfloat16)
    inputs['w_out'] = gaussian(shared[8], (MODEL_DIM, LATENT_CH), MODEL_DIM ** -0.5).astype(jnp.bfloat16)
    return inputs


def layer_norm(hidden):
    values = hidden.astype(jnp.float32)
    centered = values - jnp.mean(values, axis=-1, keepdims=True)
    variance = jnp.mean(centered * centered, axis=-1, keepdims=True)
    return centered * lax.rsqrt(variance + LN_EPS)


def modulate(hidden, shift, scale):
    return (layer_norm(hidden) * (1.0 + scale) + shift).astype(jnp.bfloat16)


def add_residual(hidden, delta):
    return (hidden.astype(jnp.float32) + delta).astype(jnp.bfloat16)


def project_qkv(normed, w_qkv):
    return jnp.einsum('pd,dshe->pshe', normed.astype(jnp.float32), w_qkv.astype(jnp.float32)).astype(jnp.bfloat16)


def spatial_frame(normed, w_qkv, w_proj):
    projected = project_qkv(normed, w_qkv).astype(jnp.float32)
    scores = jnp.einsum('qhe,khe->hqk', projected[:, 0], projected[:, 1]) * HEAD_DIM ** -0.5
    attn_probs = jax.nn.softmax(scores, axis=-1).astype(jnp.bfloat16).astype(jnp.float32)
    mixed = jnp.einsum('hqk,khe->qhe', attn_probs, projected[:, 2]).astype(jnp.bfloat16)
    return jnp.einsum('qhe,hed->qd', mixed.astype(jnp.float32), w_proj.astype(jnp.float32))


def temporal_queue(normed, w_qkv, bias, w_proj):
    projected = lax.map(lambda frame: project_qkv(frame, w_qkv), normed)
    padding = jnp.zeros((WINDOW - 1,) + projected.shape[1:], jnp.bfloat16)
    padded = jnp.concatenate([padding, projected], axis=0)
    bias_rev = bias[:, ::-1]

    def one_query(index):
        query = lax.dynamic_index_in_dim(projected, index, 0, keepdims=False)[:, 0].astype(jnp.float32)
        window_kv = lax.dynamic_slice_in_dim(padded, index, WINDOW, 0)[:, :, 1:].astype(jnp.float32)
        scores = jnp.einsum('phe,ophe->pho', query, window_kv[:, :, 0]) * HEAD_DIM ** -0.5 + bias_rev[None]
        valid = index + jnp.arange(WINDOW) >= WINDOW - 1
        scores = jnp.where(valid, scores, MASKED)
        attn_probs = jax.nn.softmax(scores, axis=-1).astype(jnp.bfloat16).astype(jnp.float32)
        mixed = jnp.einsum('pho,ophe->phe', attn_probs, window_kv[:, :, 1]).astype(jnp.bfloat16)
        return jnp.einsum('phe,hed->pd', mixed.astype(jnp.float32), w_proj.astype(jnp.float32))

    return lax.map(one_query, jnp.arange(QUEUE_LEN))


def mlp_frame(normed, w_up, w_down):
    inner = jnp.dot(normed, w_up, preferred_element_type=jnp.float32)
    activated = jax.nn.gelu(inner, approximate=True).astype(jnp.bfloat16)
    return jnp.dot(activated, w_down, preferred_element_type=jnp.float32)


def transformer_layer(hidden, layer):
    mod_layer, sp_qkv, sp_out, tm_qkv, tm_bias, tm_out, mlp_up, mlp_down = layer
    normed = modulate(hidden, mod_layer[:, 0:1], mod_layer[:, 1:2])
    hidden = add_residual(hidden, lax.map(lambda frame: spatial_frame(frame, sp_qkv, sp_out), normed))
    normed = modulate(hidden, mod_layer[:, 2:3], mod_layer[:, 3:4])
    hidden = add_residual(hidden, temporal_queue(normed, tm_qkv, tm_bias, tm_out))
    normed = modulate(hidden, mod_layer[:, 4:5], mod_layer[:, 5:6])
    hidden = add_residual(hidden, lax.map(lambda frame: mlp_frame(frame, mlp_up, mlp_down), normed))
    return hidden, None


def run_queue(latents, modulation, step_dt, noise, weights):
    w_in = weights[0]
    w_out = weights[-1]
    layer_stack = (jnp.moveaxis(modulation, 1, 0),) + tuple(weights[1:-1])

    def step(queue, noise_frame):
        hidden = jnp.dot(queue.reshape(-1, LATENT_CH).astype(jnp.bfloat16), w_in, preferred_element_type=jnp.float32)
        hidden = hidden.astype(jnp.bfloat16).reshape(QUEUE_LEN, FRAME_TOKENS, MODEL_DIM)
        hidden, unused = lax.scan(transformer_layer, hidden, layer_stack)
        normed = layer_norm(hidden).astype(jnp.bfloat16).reshape(-1, MODEL_DIM)
        velocity = jnp.dot(normed, w_out, preferred_element_type=jnp.float32).reshape(queue.shape)
        updated = queue + step_dt[:, None, None] * velocity
        shifted = jnp.concatenate([updated[1:], noise_frame[None]], axis=0)
        return shifted, updated[0]

    final, emitted = lax.scan(step, latents, noise)
    return emitted, final


def reference(latents_a, mod_a, dt_a, noise_a, latents_b, mod_b, dt_b, noise_b, w_in, sp_qkv, sp_out, tm_qkv, tm_bias, tm_out, mlp_up, mlp_down, w_out):
    weights = (w_in, sp_qkv, sp_out, tm_qkv, tm_bias, tm_out, mlp_up, mlp_down, w_out)
    emit_a, final_a = run_queue(latents_a, mod_a, dt_a, noise_a, weights)
    emit_b, final_b = run_queue(latents_b, mod_b, dt_b, noise_b, weights)
    return (emit_a, final_a, emit_b, final_b)
```

```python
import functools
import jax
import jax.numpy as jnp
from jax import lax
from jax.experimental import pallas as pl
from jax.experimental.pallas import tpu as pltpu
from jax.sharding import PartitionSpec as P

LN_EPS = 1e-6
MASKED = -1e30
LOG2E = 1.4426950408889634
F32 = jnp.float32
BF16 = jnp.bfloat16


def mm(lhs, rhs, lc, rc):
    return lax.dot_general(lhs, rhs, (((lc,), (rc,)), ((), ())), preferred_element_type=F32)


def norm_rows(x):
    centered = x - jnp.mean(x, axis=-1, keepdims=True)
    return centered * lax.rsqrt(jnp.mean(centered * centered, axis=-1, keepdims=True) + LN_EPS)


def norm_cols(x):
    centered = x - jnp.mean(x, axis=0, keepdims=True)
    return centered * lax.rsqrt(jnp.mean(centered * centered, axis=0, keepdims=True) + LN_EPS)


def pipelined(items, scores, weigh, mix, ahead=2, behind=2):
    raw, weighed = {}, {}
    count = len(items)
    for n in range(-ahead, count + behind):
        if n + ahead < count:
            raw[n + ahead] = scores(items[n + ahead])
        if 0 <= n < count:
            weighed[n] = weigh(items[n], raw.pop(n))
        if 0 <= n - behind < count:
            mix(items[n - behind], weighed.pop(n - behind))


def spatial(u, wqkv_t, wo, heads):
    rows, dim = u.shape
    half = rows // 2
    width = dim // heads
    qkv = mm(wqkv_t, u, 1, 1).astype(BF16)
    outs = {}

    def part(index, h, f):
        return qkv[index * dim + h * width:index * dim + (h + 1) * width, f * half:(f + 1) * half]

    items = [(h, f) for h in range(heads) for f in range(2)]
    keys = {item: part(1, *item).T for item in items}

    def scores(item):
        return mm(keys[item], part(0, *item), 1, 0)

    def weigh(item, s):
        p = jnp.exp2((s - jnp.max(s, axis=0, keepdims=True)) * (LOG2E * width ** -0.5))
        return p.astype(BF16), 1.0 / jnp.sum(p, axis=0, keepdims=True)

    def mix(item, weighed):
        outs[item] = (mm(part(2, *item), weighed[0], 1, 0) * weighed[1]).astype(BF16)

    pipelined(items, scores, weigh, mix)
    mixed = jnp.concatenate([jnp.concatenate([outs[h, f] for f in range(2)], axis=1) for h in range(heads)], axis=0)
    return mm(mixed, wo, 0, 0)


def pair_rows(first, second):
    rows, dim = first.shape
    both = jnp.concatenate([first.reshape(rows // 8, 1, 8, dim), second.reshape(rows // 8, 1, 8, dim)], axis=1)
    return both.reshape(2 * rows, dim)


def pair_mod(x, scale, shift):
    rows, dim = x.shape
    x = x.reshape(rows // 16, 2, 8, dim)
    return (x * scale[None, :, None, :] + shift[None, :, None, :]).reshape(rows, dim)


def stage_a(heads, z_ref, mod_ref, w_in, wqkv_t, wo, x_ref, u_ref):
    tokens = z_ref.shape[1]
    z = jnp.concatenate([z_ref[0], z_ref[1]], axis=0).astype(BF16)
    x0 = mm(z, w_in[...], 1, 0).astype(BF16).astype(F32)
    n0 = norm_rows(x0)
    u = jnp.concatenate([n0[s * tokens:(s + 1) * tokens] * (1.0 + mod_ref[s, 1:2]) + mod_ref[s, 0:1] for s in range(2)], axis=0).astype(BF16)
    x = x0 + spatial(u, wqkv_t[...], wo[...], heads)
    x = pair_rows(x[:tokens], x[tokens:]).astype(BF16)
    x_ref[0] = x
    u_ref[0] = pair_mod(norm_rows(x.astype(F32)), 1.0 + mod_ref[:, 3], mod_ref[:, 2]).astype(BF16)


def stage_t(heads, halo_ref, own_ref, wqkv_t, bias_ref, o_ref):
    dim = own_ref.shape[-1]
    width = dim // heads
    groups = own_ref.shape[1] // 16
    own = [own_ref[:, g * 16:(g + 1) * 16].reshape(-1, dim) for g in range(groups)]
    halo = [halo_ref[:, g * 16:(g + 1) * 16].reshape(-1, dim) for g in range(groups)]
    queries = own[0].shape[0]
    keys = 2 * queries
    q_all = (mm(wqkv_t[:dim], jnp.concatenate(own, axis=0), 1, 1) * width ** -0.5).astype(BF16)
    kv_all = mm(wqkv_t[dim:], jnp.concatenate([b for g in range(groups) for b in (halo[g], own[g])], axis=0), 1, 1).astype(BF16)
    sub = lax.broadcasted_iota(jnp.int32, (keys, 2 * queries), 0) % 8
    lane = lax.broadcasted_iota(jnp.int32, (keys, 2 * queries), 1) % 8
    same = sub == lane
    outs = {}
    items = [(pair, g) for pair in range(heads // 2) for g in range(groups)]
    rows = lambda pair: slice(2 * pair * width, 2 * (pair + 1) * width)
    k_rows = {(pair, g): kv_all[rows(pair), g * keys:(g + 1) * keys].T for pair, g in items}
    zero = jnp.zeros((width, queries), BF16)

    def scores(item):
        pair, g = item
        q = q_all[rows(pair), g * queries:(g + 1) * queries]
        q = jnp.concatenate([jnp.concatenate([q[:width], zero], axis=1), jnp.concatenate([zero, q[width:]], axis=1)], axis=0)
        return mm(k_rows[item], q, 1, 0)

    def weigh(item, s):
        pair, g = item
        s = s.reshape(keys // 8, 8, 2 * queries) + bias_ref[:, :, 2 * pair * queries:2 * (pair + 1) * queries]
        p = jnp.exp2((s - jnp.max(s, axis=0, keepdims=True)) * LOG2E)
        total = jnp.sum(p, axis=0)
        total = jnp.sum(jnp.where(same[:8], total, 0.0), axis=0, keepdims=True)
        return jnp.where(same, p.reshape(keys, 2 * queries), 0.0).astype(BF16), 1.0 / total

    def mix(item, weighed):
        pair, g = item
        mixed = mm(kv_all[dim + 2 * pair * width:dim + 2 * (pair + 1) * width, g * keys:(g + 1) * keys], weighed[0], 1, 0) * weighed[1]
        outs[item] = jnp.concatenate([mixed[:width, :queries], mixed[width:, queries:]], axis=0).astype(BF16)

    pipelined(items, scores, weigh, mix)
    for g in range(groups):
        o = jnp.concatenate([outs[pair, g] for pair in range(heads // 2)], axis=0)
        o_ref[:, g * 16:(g + 1) * 16] = o.T.reshape(-1, 16, dim)


def stage_m(o_ref, x_ref, mod_ref, dt_ref, z_ref, wo, w_up_t, w_down_t, w_out_t, out_ref):
    x = (x_ref[0].astype(F32) + mm(o_ref[0], wo[...], 1, 0)).astype(BF16)
    u = pair_mod(norm_rows(x.astype(F32)), 0.5 * (1.0 + mod_ref[:, 5]), 0.5 * mod_ref[:, 4]).astype(BF16)
    first = 2 * pl.program_id(0)
    tokens = x.shape[0] // 2
    h = mm(w_up_t[...], u, 1, 1)
    t = jnp.tanh(h * (1.5957691216057308 + 0.285419265090401 * (h * h)))
    h = (h + h * t).astype(BF16)
    x_t = (x.T.astype(F32) + mm(w_down_t[...], h, 1, 0)).astype(BF16).astype(F32)
    v = mm(w_out_t[...], norm_cols(x_t).astype(BF16), 1, 0)[:8].T
    v = v.reshape(tokens // 8, 2, 8, 8)
    for s in range(2):
        out_ref[s] = z_ref[s] + dt_ref[first + s] * v[:, s].reshape(tokens, 8)[:, :4]


def solution(mesh):
    group = mesh.shape['frames']
    slot_spec = P(('videos', 'frames'))
    emit_spec = P('videos', 'frames')
    whole = P()
    to_next = [(source, source + 1) for source in range(group - 1)]
    to_prev = [(source + 1, source) for source in range(group - 1)]

    def local(latents_a, mod_a, dt_a, noise_a, latents_b, mod_b, dt_b, noise_b, w_in, sp_qkv, sp_out, tm_qkv, tm_bias, tm_out, mlp_up, mlp_down, w_out):
        position = lax.axis_index('frames')
        slots, tokens, channels = latents_a.shape
        dim = w_in.shape[1]
        heads = tm_bias.shape[1]
        window = tm_bias.shape[-1]
        pairs = slots // 2
        full = lambda a: pl.BlockSpec(a.shape, lambda i: (0,) * a.ndim, pipeline_mode=pl.Buffered(1))
        sp_t = jnp.transpose(sp_qkv[0], (1, 2, 3, 0)).reshape(3 * dim, dim)
        tm_t = jnp.transpose(tm_qkv[0], (1, 2, 3, 0)).reshape(3 * dim, dim)
        sp_o = sp_out[0].reshape(dim, dim)
        tm_o = tm_out[0].reshape(dim, dim)
        up_t = mlp_up[0].T
        down_t = mlp_down[0].T
        out_t = jnp.pad(w_out.T, ((0, 16 - channels), (0, 0)))
        offset = jnp.arange(slots)[None, :] + slots - jnp.arange(2 * slots)[:, None]
        keep = (offset >= 0) & (offset < window) & ((jnp.arange(2 * slots)[:, None] >= slots) | (position > 0))
        table = jnp.where(keep[:, None], jnp.take(tm_bias[0], jnp.clip(offset, 0, window - 1), axis=1).transpose(1, 0, 2), MASKED)
        table = jnp.broadcast_to(table[:, None, :, :, None], (2 * slots, 8, heads, slots, 8)).reshape(2 * slots, 8, heads * slots * 8)
        params = pltpu.CompilerParams(vmem_limit_bytes=60 * 1024 * 1024)
        pair_block = lambda: pl.BlockSpec((1, 2 * tokens, dim), lambda i: (i, 0, 0))
        slot_block = lambda *rest: pl.BlockSpec((2, *rest), lambda i: (i,) + (0,) * len(rest))
        act = jax.ShapeDtypeStruct((pairs, 2 * tokens, dim), BF16)

        def call_a(z, mod):
            return pl.pallas_call(
                functools.partial(stage_a, heads), grid=(pairs,),
                in_specs=[slot_block(tokens, channels), slot_block(6, dim), full(w_in), full(sp_t), full(sp_o)],
                out_specs=[pair_block(), pair_block()], out_shape=[act, act], compiler_params=params, name='stage_a',
                cost_estimate=pl.CostEstimate(flops=20 * 10**9, bytes_accessed=12 * 10**6, transcendentals=0),
            )(z, mod, w_in, sp_t, sp_o)

        def call_t(halo, own):
            block = lambda: pl.BlockSpec((pairs, 32, dim), lambda i: (0, i, 0))
            return pl.pallas_call(
                functools.partial(stage_t, heads), grid=(tokens // 16,),
                in_specs=[block(), block(), full(tm_t), full(table)],
                out_specs=block(), out_shape=act, compiler_params=params, name='stage_t',
                cost_estimate=pl.CostEstimate(flops=20 * 10**9, bytes_accessed=12 * 10**6, transcendentals=0),
            )(halo, own, tm_t, table)

        def call_m(o, x, mod, dt, z):
            return pl.pallas_call(
                stage_m, grid=(pairs,),
                in_specs=[pair_block(), pair_block(), slot_block(6, dim), pl.BlockSpec(memory_space=pltpu.SMEM), slot_block(tokens, channels),
                          full(tm_o), full(up_t), full(down_t), full(out_t)],
                out_specs=slot_block(tokens, channels), out_shape=jax.ShapeDtypeStruct((slots, tokens, channels), F32), compiler_params=params, name='stage_m',
                cost_estimate=pl.CostEstimate(flops=20 * 10**9, bytes_accessed=12 * 10**6, transcendentals=0),
            )(o, x, mod, dt, z, tm_o, up_t, down_t, out_t)

        mods = [mod_a[:, 0], mod_b[:, 0]]
        dts = [dt_a, dt_b]

        def step(queues, noise):
            front = [call_a(queues[n], mods[n]) for n in range(2)]
            halos = [lax.ppermute(front[n][1], 'frames', to_next) for n in range(2)]
            new, emitted = [], []
            for n in range(2):
                mixed = call_t(halos[n], front[n][1])
                updated = call_m(mixed, front[n][0], mods[n], dts[n], queues[n])
                from_next = lax.ppermute(updated[0], 'frames', to_prev)
                incoming = jnp.where(position == group - 1, noise[n], from_next)
                new.append(jnp.concatenate([updated[1:], incoming[None]], axis=0))
                emitted.append(updated[0])
            return tuple(new), jnp.stack(emitted)

        queues, emit = lax.scan(step, (latents_a, latents_b), (noise_a, noise_b))
        emit = jnp.moveaxis(emit, 1, 0).reshape(-1, tokens, channels)
        emit = lax.psum_scatter(jnp.where(position == 0, emit, 0.0), 'frames', scatter_dimension=1, tiled=True)
        half = emit.shape[0] // 2
        return emit[:half], queues[0], emit[half:], queues[1]

    return jax.shard_map(local, mesh=mesh, in_specs=(slot_spec, slot_spec, slot_spec, P('videos'), slot_spec, slot_spec, slot_spec, P('videos')) + (whole,) * 9, out_specs=(emit_spec, slot_spec, emit_spec, slot_spec), check_vma=False)
```

```python
import functools
import jax
import jax.numpy as jnp
from jax import lax
from jax.experimental import pallas as pl
from jax.experimental.pallas import tpu as pltpu
from jax.sharding import PartitionSpec as P

LN_EPS = 1e-6
MASKED = -1e30
LOG2E = 1.4426950408889634
F32 = jnp.float32
BF16 = jnp.bfloat16


def mm(lhs, rhs, lc, rc):
    return lax.dot_general(lhs, rhs, (((lc,), (rc,)), ((), ())), preferred_element_type=F32)


def norm(x, axis):
    centered = x - jnp.mean(x, axis=axis, keepdims=True)
    return centered * lax.rsqrt(jnp.mean(centered * centered, axis=axis, keepdims=True) + LN_EPS)


def pipelined(items, scores, weigh, mix, ahead=2, behind=2):
    raw, weighed = {}, {}
    count = len(items)
    for n in range(-ahead, count + behind):
        if n + ahead < count:
            raw[n + ahead] = scores(items[n + ahead])
        if 0 <= n < count:
            weighed[n] = weigh(items[n], raw.pop(n))
        if 0 <= n - behind < count:
            mix(items[n - behind], weighed.pop(n - behind))


def spatial(u, wqkv_t, wo, heads):
    rows, dim = u.shape
    half = rows // 2
    width = dim // heads
    qkv = mm(wqkv_t, u, 1, 1).astype(BF16)
    outs = {}

    def part(index, h, f):
        return qkv[index * dim + h * width:index * dim + (h + 1) * width, f * half:(f + 1) * half]

    items = [(h, f) for h in range(heads) for f in range(2)]
    keys = {item: part(1, *item).T for item in items}

    def scores(item):
        return mm(keys[item], part(0, *item), 1, 0)

    def weigh(item, s):
        p = jnp.exp2((s - jnp.max(s, axis=0, keepdims=True)) * (LOG2E * width ** -0.5))
        return p.astype(BF16), 1.0 / jnp.sum(p, axis=0, keepdims=True)

    def mix(item, weighed):
        outs[item] = (mm(part(2, *item), weighed[0], 1, 0) * weighed[1]).astype(BF16)

    pipelined(items, scores, weigh, mix)
    mixed = jnp.concatenate([jnp.concatenate([outs[h, f] for f in range(2)], axis=1) for h in range(heads)], axis=0)
    return mm(mixed, wo, 0, 0)


def pair_rows(first, second):
    rows, dim = first.shape
    both = jnp.concatenate([first.reshape(rows // 8, 1, 8, dim), second.reshape(rows // 8, 1, 8, dim)], axis=1)
    return both.reshape(2 * rows, dim)


def pair_mod(x, scale, shift):
    rows, dim = x.shape
    x = x.reshape(rows // 16, 2, 8, dim)
    return (x * scale[None, :, None, :] + shift[None, :, None, :]).reshape(rows, dim)


def stage_a(z, mod, w_in, wqkv_t, wo, heads):
    rows = z.shape[0] // 2
    x0 = mm(z.astype(BF16), w_in, 1, 0).astype(BF16).astype(F32)
    n0 = norm(x0, -1)
    u = jnp.concatenate([n0[s * rows:(s + 1) * rows] * mod[s, 1:2] + mod[s, 0:1] for s in range(2)], axis=0).astype(BF16)
    x = x0 + spatial(u, wqkv_t, wo, heads)
    x = pair_rows(x[:rows], x[rows:]).astype(BF16)
    return x, pair_mod(norm(x.astype(F32), -1), mod[:, 3], mod[:, 2]).astype(BF16)


def stage_t(us, wqkv_t, bias_ref, heads):
    keys, dim = us[0].shape
    groups = len(us)
    queries = keys // 2
    width = dim // heads
    q_all = (mm(wqkv_t[:dim], jnp.concatenate([u[queries:] for u in us], axis=0), 1, 1) * width ** -0.5).astype(BF16)
    kv_all = mm(wqkv_t[dim:], jnp.concatenate(us, axis=0), 1, 1).astype(BF16)
    sub = lax.broadcasted_iota(jnp.int32, (keys, 2 * queries), 0) % 8
    lane = lax.broadcasted_iota(jnp.int32, (keys, 2 * queries), 1) % 8
    same = sub == lane
    outs = {}
    items = [(pair, g) for pair in range(heads // 2) for g in range(groups)]
    rows = lambda pair: slice(2 * pair * width, 2 * (pair + 1) * width)
    k_rows = {(pair, g): kv_all[rows(pair), g * keys:(g + 1) * keys].T for pair, g in items}
    zero = jnp.zeros((width, queries), BF16)

    def scores(item):
        pair, g = item
        q = q_all[rows(pair), g * queries:(g + 1) * queries]
        q = jnp.concatenate([jnp.concatenate([q[:width], zero], axis=1), jnp.concatenate([zero, q[width:]], axis=1)], axis=0)
        return mm(k_rows[item], q, 1, 0)

    def weigh(item, s):
        pair, g = item
        s = s.reshape(keys // 8, 8, 2 * queries) + bias_ref[:, :, 2 * pair * queries:2 * (pair + 1) * queries]
        p = jnp.exp2((s - jnp.max(s, axis=0, keepdims=True)) * LOG2E)
        total = jnp.sum(p, axis=0)
        total = jnp.sum(jnp.where(same[:8], total, 0.0), axis=0, keepdims=True)
        return jnp.where(same, p.reshape(keys, 2 * queries), 0.0).astype(BF16), 1.0 / total

    def mix(item, weighed):
        pair, g = item
        mixed = mm(kv_all[dim + 2 * pair * width:dim + 2 * (pair + 1) * width, g * keys:(g + 1) * keys], weighed[0], 1, 0) * weighed[1]
        outs[item] = jnp.concatenate([mixed[:width, :queries], mixed[width:, queries:]], axis=0).astype(BF16)

    pipelined(items, scores, weigh, mix)
    return [jnp.concatenate([outs[pair, g] for pair in range(heads // 2)], axis=0).T for g in range(groups)]


def stage_m(o, x, mod, wo, w_up_t, w_down_t, w_out_t):
    x = (x.astype(F32) + mm(o, wo, 1, 0)).astype(BF16)
    u = pair_mod(norm(x.astype(F32), -1), mod[:, 5], mod[:, 4]).astype(BF16)
    tokens = x.shape[0] // 2
    h = mm(w_up_t, u, 1, 1)
    t = jnp.tanh(h * (1.5957691216057308 + 0.285419265090401 * (h * h)))
    h = (h + h * t).astype(BF16)
    x_t = (x.T.astype(F32) + mm(w_down_t, h, 1, 0)).astype(BF16).astype(F32)
    v = mm(w_out_t, norm(x_t, 0).astype(BF16), 1, 0)[:8].T.reshape(tokens // 8, 2, 8, 8)
    return [v[:, s].reshape(tokens, 8) for s in range(2)]


def kernel(group, heads, lat_a, lat_b, noise_a, noise_b, mod_a, mod_b, dt_a, dt_b, table, w_in, sp_t, sp_o, tm_t, tm_o, up_t, down_t, out_t,
           fin_a, fin_b, emit_a, emit_b,
           z_buf, z_in, z_noise, mod_buf, dt_buf, x_buf, u_buf, o_buf, e_buf,
           send_sem, recv_sem, free_sem, z_send, z_recv, e_send, e_recv):
    slots, channels, tokens = lat_a.shape
    steps = noise_a.shape[0]
    pairs = slots // 2
    me = lax.axis_index('frames')
    last = group - 1
    nxt = jnp.minimum(me + 1, last)
    prv = jnp.maximum(me - 1, 0)
    mesh_id = pl.DeviceIdType.MESH
    share = tokens // group

    def halo_copy(n, f):
        return pltpu.make_async_remote_copy(
            src_ref=u_buf.at[n, pairs + f], dst_ref=u_buf.at[n, f], send_sem=send_sem.at[n, f], recv_sem=recv_sem.at[n, f],
            device_id={'frames': nxt}, device_id_type=mesh_id)

    def z_copy(n):
        return pltpu.make_async_remote_copy(
            src_ref=z_buf.at[n, slots], dst_ref=z_in.at[n], send_sem=z_send.at[n], recv_sem=z_recv.at[n],
            device_id={'frames': prv}, device_id_type=mesh_id)

    def e_copy(n, t, d):
        return pltpu.make_async_remote_copy(
            src_ref=z_buf.at[n, slots, pl.ds(pl.multiple_of(d * share, 8), share)], dst_ref=e_buf.at[n, t],
            send_sem=e_send.at[n, d], recv_sem=e_recv.at[n, t], device_id={'frames': d}, device_id_type=mesh_id)

    barrier = pltpu.get_barrier_semaphore()

    @pl.when(me > 0)
    def _():
        pl.semaphore_signal(barrier, inc=1, device_id={'frames': prv}, device_id_type=mesh_id)

    @pl.when(me > 1)
    def _():
        pl.semaphore_signal(barrier, inc=1, device_id={'frames': 0}, device_id_type=mesh_id)

    @pl.when(me < last)
    def _():
        pl.semaphore_signal(barrier, inc=1, device_id={'frames': nxt}, device_id_type=mesh_id)

    for n, (lat, mod, dt, noise) in enumerate(((lat_a, mod_a, dt_a, noise_a), (lat_b, mod_b, dt_b, noise_b))):
        @pl.loop(0, slots)
        def _(k):
            z_buf[n, k] = lat[k].T
            m = mod[k]
            odd = lax.broadcasted_iota(jnp.int32, m.shape, 0) % 2
            m = jnp.where(odd == 1, 1.0 + m, m)
            mod_buf[n, k] = jnp.where(lax.broadcasted_iota(jnp.int32, m.shape, 0) >= 4, 0.5 * m, m)
            dt_buf[n, k] = dt[k]

        @pl.loop(0, steps)
        def _(t):
            z_noise[n, t] = noise[t].T

    @pl.when(me == 0)
    def _():
        @pl.loop(0, pairs)
        def _(f):
            for n in range(2):
                u_buf[n, f] = jnp.zeros(u_buf.shape[2:], BF16)

    pl.semaphore_wait(barrier, jnp.where(me == 0, last, jnp.where(me == last, 1, 2)))

    @pl.loop(0, steps)
    def _(t):
        @pl.loop(0, 2)
        def _(n):
            @pl.when((t > 0) & (me < last))
            def _():
                z_copy(n).wait_recv()
                z_buf[n, slots - 1] = z_in[n]

            @pl.when((t > 0) & (me == last))
            def _():
                z_buf[n, slots - 1] = z_noise[n, t - 1]

            @pl.when((t > 0) & (me < last))
            def _():
                pl.semaphore_wait(free_sem.at[n], 1)

            @pl.loop(0, pairs)
            def _(f):
                @pl.when((t > 0) & (me < last))
                def _():
                    halo_copy(n, f).wait_send()

                z = jnp.concatenate([z_buf[n, 2 * f], z_buf[n, 2 * f + 1]], axis=0)
                x, u = stage_a(z, mod_buf[n, pl.ds(2 * f, 2)], w_in[...], sp_t[...], sp_o[...], heads)
                x_buf[n, f] = x
                u_buf[n, pairs + f] = u

                @pl.when((f > 0) & (me < last))
                def _():
                    halo_copy(n, f - 1).start()

            @pl.when(me < last)
            def _():
                halo_copy(n, pairs - 1).start()

        @pl.loop(0, 2)
        def _(n):
            @pl.when(me > 0)
            def _():
                @pl.loop(0, pairs)
                def _(f):
                    halo_copy(n, f).wait_recv()

            @pl.loop(0, tokens // 16)
            def _(i):
                rows = pl.ds(pl.multiple_of(i * 32, 32), 32)
                both = u_buf[n, :, rows]
                mixed = stage_t([both[:, g * 16:(g + 1) * 16].reshape(-1, both.shape[-1]) for g in range(2)], tm_t, table, heads)
                o_buf[:, rows] = jnp.concatenate([m.reshape(pairs, 16, -1) for m in mixed], axis=1)

            @pl.when((t < steps - 1) & (me > 0))
            def _():
                pl.semaphore_signal(free_sem.at[n], inc=1, device_id={'frames': prv}, device_id_type=mesh_id)

            @pl.when((t > 0) & (me > 0))
            def _():
                z_copy(n).wait_send()

            @pl.when((t > 0) & (me == 0))
            def _():
                @pl.loop(1, group)
                def _(d):
                    e_copy(n, t - 1, d).wait_send()

            @pl.loop(0, pairs)
            def _(f):
                v = stage_m(o_buf[f], x_buf[n, f], mod_buf[n, pl.ds(2 * f, 2)], tm_o[...], up_t[...], down_t[...], out_t[...])
                new = [z_buf[n, 2 * f + s] + dt_buf[n, 2 * f + s] * v[s][:, :channels] for s in range(2)]
                z_buf[n, lax.rem(2 * f + slots, slots + 1)] = new[0]
                z_buf[n, 2 * f] = new[1]

                @pl.when((f == 1) & (me > 0))
                def _():
                    z_copy(n).start()

                @pl.when((f == 1) & (me == 0))
                def _():
                    e_buf[n, t] = z_buf[n, slots, :share]

                    @pl.loop(1, group)
                    def _(d):
                        e_copy(n, t, d).start()

    @pl.loop(0, 2)
    def _(n):
        @pl.when(me < last)
        def _():
            z_copy(n).wait_recv()
            z_buf[n, slots - 1] = z_in[n]

            @pl.loop(0, pairs)
            def _(f):
                halo_copy(n, f).wait_send()

        @pl.when(me == last)
        def _():
            z_buf[n, slots - 1] = z_noise[n, steps - 1]

        @pl.when(me > 0)
        def _():
            z_copy(n).wait_send()

            @pl.loop(0, steps)
            def _(t):
                e_copy(n, t, 0).wait_recv()

        @pl.when(me == 0)
        def _():
            @pl.loop(1, group)
            def _(d):
                e_copy(n, steps - 1, d).wait_send()

    for n, (fin, emit) in enumerate(((fin_a, emit_a), (fin_b, emit_b))):
        @pl.loop(0, slots)
        def _(k):
            fin[k] = z_buf[n, k].T

        emit[...] = e_buf[n]


def solution(mesh):
    group = mesh.shape['frames']
    slot_spec = P(('videos', 'frames'))
    emit_spec = P('videos', 'frames')
    whole = P()

    def local(latents_a, mod_a, dt_a, noise_a, latents_b, mod_b, dt_b, noise_b, w_in, sp_qkv, sp_out, tm_qkv, tm_bias, tm_out, mlp_up, mlp_down, w_out):
        position = lax.axis_index('frames')
        slots, tokens, channels = latents_a.shape
        steps = noise_a.shape[0]
        dim = w_in.shape[1]
        heads = tm_bias.shape[1]
        window = tm_bias.shape[-1]
        pairs = slots // 2
        sp_t = jnp.transpose(sp_qkv[0], (1, 2, 3, 0)).reshape(3 * dim, dim)
        tm_t = jnp.transpose(tm_qkv[0], (1, 2, 3, 0)).reshape(3 * dim, dim)
        out_t = jnp.pad(w_out.T, ((0, 16 - channels), (0, 0)))
        offset = jnp.arange(slots)[None, :] + slots - jnp.arange(2 * slots)[:, None]
        keep = (offset >= 0) & (offset < window) & ((jnp.arange(2 * slots)[:, None] >= slots) | (position > 0))
        table = jnp.where(keep[:, None], jnp.take(tm_bias[0], jnp.clip(offset, 0, window - 1), axis=1).transpose(1, 0, 2), MASKED)
        table = jnp.broadcast_to(table[:, None, :, :, None], (2 * slots, 8, heads, slots, 8)).reshape(2 * slots, 8, heads * slots * 8)
        swap = lambda a: jnp.swapaxes(a, 1, 2)
        vmem = pl.BlockSpec(memory_space=pltpu.VMEM)
        smem = pl.BlockSpec(memory_space=pltpu.SMEM)
        dma = pltpu.SemaphoreType.DMA
        fin_a, fin_b, emit_a, emit_b = pl.pallas_call(
            functools.partial(kernel, group, heads),
            in_specs=[vmem] * 6 + [smem] * 2 + [vmem] * 9,
            out_specs=[vmem] * 4,
            out_shape=[jax.ShapeDtypeStruct((slots, channels, tokens), F32)] * 2 + [jax.ShapeDtypeStruct((steps, tokens // group, channels), F32)] * 2,
            scratch_shapes=[
                pltpu.VMEM((2, slots + 1, tokens, channels), F32),
                pltpu.VMEM((2, tokens, channels), F32),
                pltpu.VMEM((2, steps, tokens, channels), F32),
                pltpu.VMEM((2, slots, 6, dim), F32),
                pltpu.SMEM((2, slots), F32),
                pltpu.VMEM((2, pairs, 2 * tokens, dim), BF16),
                pltpu.VMEM((2, 2 * pairs, 2 * tokens, dim), BF16),
                pltpu.VMEM((pairs, 2 * tokens, dim), BF16),
                pltpu.VMEM((2, steps, tokens // group, channels), F32),
                dma((2, pairs)), dma((2, pairs)), pltpu.SemaphoreType.REGULAR((2,)),
                dma((2,)), dma((2,)), dma((2, group)), dma((2, steps)),
            ],
            compiler_params=pltpu.CompilerParams(collective_id=0, has_side_effects=True, vmem_limit_bytes=62 * 1024 * 1024),
            name='queues',
        )(swap(latents_a), swap(latents_b), swap(noise_a), swap(noise_b), mod_a[:, 0], mod_b[:, 0], dt_a, dt_b, table, w_in,
          sp_t, sp_out[0].reshape(dim, dim), tm_t, tm_out[0].reshape(dim, dim), mlp_up[0].T, mlp_down[0].T, out_t)
        return emit_a, swap(fin_a), emit_b, swap(fin_b)

    return jax.shard_map(local, mesh=mesh, in_specs=(slot_spec, slot_spec, slot_spec, P('videos'), slot_spec, slot_spec, slot_spec, P('videos')) + (whole,) * 9, out_specs=(emit_spec, slot_spec, emit_spec, slot_spec), check_vma=False)
```
